32 devices in a mesh: dp: 8 (over z, x), mp: 4 (over y, core).
Axes of the slice: x: 2, y: 2, z: 4, core: 2. Of those that a mesh axis runs over, the one named last changes fastest.
Arguments:
- tokens: bfloat16 [16384, 1024], P(('dp', 'mp')), may hold values from -6 to 6
- segments: int32 [8, 2048], P('dp'), may hold values from 0 to 7, never falling along the last dimension, each value on 1 to 512 neighbouring positions
- attn_norm_gain: float32 [1024], replicated, may hold values from 0.1 to 1.9
- attn_norm_bias: float32 [1024], replicated, may hold values from -3 to 3
- query_weight: bfloat16 [1024, 1024], P(None, 'mp'), may hold values from -0.1875 to 0.1875
- key_weight: bfloat16 [1024, 1024], P(None, 'mp'), may hold values from -0.1875 to 0.1875
- value_weight: bfloat16 [1024, 1024], P(None, 'mp'), may hold values from -0.1875 to 0.1875
- output_weight: bfloat16 [1024, 1024], P('mp'), may hold values from -1.5 to 1.5
- mlp_norm_gain: float32 [1024], replicated, may hold values from 0.1 to 1.9
- mlp_norm_bias: float32 [1024], replicated, may hold values from -3 to 3
- gate_weight: bfloat16 [1024, 4096], P(None, 'mp'), may hold values from -0.1875 to 0.1875
- up_weight: bfloat16 [1024, 4096], P(None, 'mp'), may hold values from -0.1875 to 0.1875
- down_weight: bfloat16 [4096, 1024], P('mp'), may hold values from -0.125 to 0.125
- grad_out: bfloat16 [16384, 1024], P(('dp', 'mp')), may hold values from -6 to 6
Outputs:
- block_out: bfloat16 [16384, 1024], P(('dp', 'mp'))
- grad_tokens: float32 [16384, 1024], P(('dp', 'mp'))
- grad_attn_norm_gain: float32 [1024], replicated
- grad_attn_norm_bias: float32 [1024], replicated
- grad_query_weight: float32 [1024, 1024], P(None, 'mp')
- grad_key_weight: float32 [1024, 1024], P(None, 'mp')
- grad_value_weight: float32 [1024, 1024], P(None, 'mp')
- grad_output_weight: float32 [1024, 1024], P('mp')
- grad_mlp_norm_gain: float32 [1024], replicated
- grad_mlp_norm_bias: float32 [1024], replicated
- grad_gate_weight: float32 [1024, 4096], P(None, 'mp')
- grad_up_weight: float32 [1024, 4096], P(None, 'mp')
- grad_down_weight: float32 [4096, 1024], P('mp')
The draws below stay inside these ranges and needn't reach their ends.
Inputs may be any that keep to these rules, and one draw needn't show every extreme that they name: `segments`: within each row of 2048 tokens the window numbers start at 0, never fall, and each of the 8 numbers holds 1 to 512 tokens.
All inputs are finite; a program needn't handle non-finite values.
Results may differ from the reference program's by a relative error of at most 0.014.
The reference program's roundings to bfloat16 on the way count: a program that leaves them out, or rounds other values in their place, can miss the bound.
Values may be sent and summed in bfloat16 or wider, within the bound.
A program may use at most 192 MiB of HBM per device.

```python
import math
import jax
import jax.numpy as jnp
import numpy as np
from jax import lax

D = 1024
HEADS = 16
HEAD_DIM = 64
FF = 4096
SEQ = 2048
WINDOWS = 8
QBLK = 512
NROWS = 8
TOKENS = 16384


def level_of(stream_key, shape, cuts, smallest, high):
    loudness, own = 1.0, jax.random.fold_in(stream_key, 6)
    for dim, shards_of in cuts:
        draws = jnp.exp(jax.random.uniform(jax.random.fold_in(own, dim), (shards_of,), jnp.float32, smallest / len(cuts), high / len(cuts)))
        loudness = loudness * jnp.repeat(draws, shape[dim] // shards_of).reshape([-1 if axis == dim else 1 for axis in range(len(shape))])
    return loudness


def profile(count, total, limit, skew):
    loads = [(1 << 20) // math.isqrt(rank ** skew) + 1 for rank in range(2, count + 1)]
    rest, counts = total - limit - (count - 1), [1] * (count - 1)
    while rest > 0:
        candidates = [i for i in range(count - 1) if counts[i] < limit]
        whole, budget = sum([loads[i] for i in candidates]), rest
        for i in candidates:
            addition = min(limit - counts[i], max(1, budget * loads[i] // whole), rest)
            counts[i] = counts[i] + addition
            rest = rest - addition
    return np.array([limit] + counts)


def ragged_sizes(key, count, total, most, slope):
    if count == 2:
        one = jax.random.randint(key, (), max(1, total - most), min(most, total - 1) + 1)
        return jnp.stack([one, total - one])
    sizes = jnp.asarray(profile(count, total, most, slope), jnp.int32)
    pairs = (count - 1) // 2
    source_of, taker = sizes[1:1 + 2 * pairs:2], sizes[2:2 + 2 * pairs:2]
    room = jnp.minimum(source_of - 1, most - taker)
    shifted = jax.random.randint(jax.random.fold_in(key, 1), (pairs,), 0, 1 << 20) % (room + 1)
    sizes = sizes.at[1:1 + 2 * pairs:2].set(source_of - shifted).at[2:2 + 2 * pairs:2].set(taker + shifted)
    return sizes[jax.random.permutation(jax.random.fold_in(key, 2), count)]


def normal_values(stream_key, extent, width, bound, split=(), kind=jnp.bfloat16):
    values = width * jax.random.normal(stream_key, extent, jnp.float32)
    if split:
        values = values * level_of(stream_key, extent, split, -0.22, 0.18)
    return jnp.clip(values, -bound, bound).astype(kind)


def setup_inputs(seed: int = 0) -> dict:
    arg_keys = jax.random.split(jax.random.key(seed), 15)
    return {
        "tokens": normal_values(arg_keys[0], (TOKENS, D), 1.0, 6.0, ((0, 32),)),
        "segments": jax.vmap(lambda own: jnp.searchsorted(jnp.cumsum(ragged_sizes(own, WINDOWS, SEQ, SEQ // 4, 1)), jnp.arange(SEQ), side="right"))(jax.random.split(arg_keys[1], NROWS)).reshape((NROWS, SEQ)).astype(jnp.int32),
        "attn_norm_gain": jnp.clip(1.0 + 0.18 * jax.random.normal(arg_keys[2], (D,), jnp.float32), 0.1, 1.9),
        "attn_norm_bias": normal_values(arg_keys[3], (D,), 0.5, 3.0, (), jnp.float32),
        "query_weight": normal_values(arg_keys[4], (D, D), D ** -0.5, 0.1875, ((1, 4),)),
        "key_weight": normal_values(arg_keys[5], (D, D), D ** -0.5, 0.1875, ((1, 4),)),
        "value_weight": normal_values(arg_keys[6], (D, D), D ** -0.5, 0.1875, ((1, 4),)),
        "output_weight": normal_values(arg_keys[7], (D, D), (D // 64) ** -0.5, 1.5, ((0, 4),)),
        "mlp_norm_gain": jnp.clip(1.0 + 0.18 * jax.random.normal(arg_keys[8], (D,), jnp.float32), 0.1, 1.9),
        "mlp_norm_bias": normal_values(arg_keys[9], (D,), 0.5, 3.0, (), jnp.float32),
        "gate_weight": normal_values(arg_keys[10], (D, FF), D ** -0.5, 0.1875, ((1, 4),)),
        "up_weight": normal_values(arg_keys[11], (D, FF), D ** -0.5, 0.1875, ((1, 4),)),
        "down_weight": normal_values(arg_keys[12], (FF, D), (FF // 2) ** -0.5, 0.125, ((0, 4),)),
        "grad_out": normal_values(arg_keys[13], (TOKENS, D), 1.0, 6.0, ((0, 32),)),
    }


@jax.custom_vjp
def low(v):
    return lax.optimization_barrier(v.astype(jnp.bfloat16)).astype(jnp.float32)

@jax.custom_vjp
def low_back(v):
    return v

def low_keep(v):
    return (low(v), None)

def low_pass(kept, grad):
    return (grad,)

def back_keep(v):
    return (v, None)

def back_low(kept, grad):
    return (low(grad),)
low.defvjp(low_keep, low_pass)
low_back.defvjp(back_keep, back_low)

def matmul(left, right):
    return jnp.dot(left, right, precision=lax.Precision.HIGHEST, preferred_element_type=jnp.float32)

def layer_norm(values, gain, shift):
    center = values - lax.optimization_barrier(jnp.mean(values, axis=-1, keepdims=True))
    variance = lax.optimization_barrier(jnp.mean(center * center, axis=-1, keepdims=True))
    return center * lax.rsqrt(variance + 1e-05) * gain + shift

def rotary_tables(segment_row):
    places = jnp.arange(SEQ, dtype=jnp.int32)
    changes = jnp.concatenate([jnp.ones((1,), jnp.int32), (segment_row[1:] != segment_row[:-1]).astype(jnp.int32)])
    starts = lax.cummax(jnp.where(changes > 0, places, 0), axis=0)
    position = (places - starts).astype(jnp.float32)
    half_dim = HEAD_DIM // 2
    frequency = 10000.0 ** (-2.0 * jnp.arange(half_dim, dtype=jnp.float32) / HEAD_DIM)
    angles = position[:, None] * frequency[None, :]
    cosine_table = jnp.concatenate([jnp.cos(angles), jnp.cos(angles)], axis=1)
    sine_table = jnp.concatenate([jnp.sin(angles), jnp.sin(angles)], axis=1)
    return (cosine_table, sine_table)

def rotate(values, cosine_table, sine_table):
    half_dim = HEAD_DIM // 2
    turned = jnp.concatenate([-values[..., half_dim:], values[..., :half_dim]], axis=-1)
    return values * cosine_table[:, None, :] + turned * sine_table[:, None, :]

def layer_row(row_data, segment_row, parameters):
    attn_gain, attn_shift, query_w, key_w, value_w, output_w, mlp_gain, mlp_shift, gate_w, up_w, down_w = parameters
    cosine_table, sine_table = rotary_tables(segment_row)
    normed = low(layer_norm(row_data, attn_gain, attn_shift))
    queries = low_back(matmul(normed, query_w)).reshape(SEQ, HEADS, HEAD_DIM)
    queries = low(rotate(queries, cosine_table, sine_table))
    key_act = low_back(matmul(normed, key_w)).reshape(SEQ, HEADS, HEAD_DIM)
    key_act = low(rotate(key_act, cosine_table, sine_table))
    value_act = low(low_back(matmul(normed, value_w))).reshape(SEQ, HEADS, HEAD_DIM)
    score_scale = HEAD_DIM ** (-0.5)

    def attend_block(offset):
        query_block = lax.dynamic_slice_in_dim(queries, offset, QBLK, 0)
        query_seg = lax.dynamic_slice_in_dim(segment_row, offset, QBLK, 0)
        raw_score = low_back(jnp.einsum('qhd,khd->hqk', query_block, key_act, precision=lax.Precision.HIGHEST))
        same_window = query_seg[:, None] == segment_row[None, :]
        scores = jnp.where(same_window[None], raw_score * score_scale, -1e+30)
        row_max = lax.optimization_barrier(jnp.max(scores, axis=-1, keepdims=True))
        log_total = row_max + jnp.log(lax.optimization_barrier(jnp.sum(jnp.exp(scores - row_max), axis=-1, keepdims=True)))
        attn_prob = jnp.exp(scores - log_total)
        return jnp.einsum('hqk,khd->qhd', low(attn_prob), value_act, precision=lax.Precision.HIGHEST)
    offsets = jnp.arange(SEQ // QBLK, dtype=jnp.int32) * QBLK
    head_out = lax.map(jax.checkpoint(attend_block), offsets).reshape(SEQ, D)
    head_out = low(low_back(head_out))
    middle = row_data + low_back(matmul(head_out, output_w))
    mlp_normed = low(layer_norm(middle, mlp_gain, mlp_shift))
    gate_act = low_back(matmul(mlp_normed, gate_w))
    up_act = low_back(matmul(mlp_normed, up_w))
    hidden = low(gate_act * jax.nn.sigmoid(gate_act) * up_act)
    return middle + low_back(matmul(hidden, down_w))

def reference(tokens, segments, attn_norm_gain, attn_norm_bias, query_weight, key_weight, value_weight, output_weight, mlp_norm_gain, mlp_norm_bias, gate_weight, up_weight, down_weight, grad_out):
    parameters = tuple((weight.astype(jnp.float32) for weight in (attn_norm_gain, attn_norm_bias, query_weight, key_weight, value_weight, output_weight, mlp_norm_gain, mlp_norm_bias, gate_weight, up_weight, down_weight)))
    row_inputs = tokens.astype(jnp.float32).reshape(NROWS, SEQ, D)
    row_cotangents = grad_out.astype(jnp.float32).reshape(NROWS, SEQ, D)

    def row_step(totals, element):
        row_data, segment_row, cotangent = element
        result, pullback = jax.vjp(lambda inner, weights: layer_row(inner, segment_row, weights), row_data, parameters)
        grad_row, grad_params = pullback(cotangent)
        totals = jax.tree.map(lambda first_sum, second_sum: first_sum + second_sum, totals, grad_params)
        return (totals, (result.astype(jnp.bfloat16), grad_row))
    zero_grads = jax.tree.map(jnp.zeros_like, parameters)
    totals, (row_outs, row_grads) = lax.scan(row_step, zero_grads, (row_inputs, segments, row_cotangents))
    return (row_outs.reshape(TOKENS, D), row_grads.reshape(TOKENS, D), totals[0], totals[1], totals[2], totals[3], totals[4], totals[5], totals[6], totals[7], totals[8], totals[9], totals[10])
```

```python
import functools
import jax
import jax.numpy as jnp
from jax import lax
from jax.experimental import pallas as pl
from jax.experimental.pallas import tpu as pltpu
from jax.sharding import PartitionSpec as P

HEAD_DIM = 64
QT = 128
KT = 256
LANES = 128

epsilon = 1e-05


def nn(left, right):
    return lax.dot_general(left, right, (((1,), (0,)), ((), ())), preferred_element_type=jnp.float32)


def nt(left, right):
    return lax.dot_general(left, right, (((1,), (1,)), ((), ())), preferred_element_type=jnp.float32)


def tn(left, right):
    return lax.dot_general(left, right, (((0,), (0,)), ((), ())), preferred_element_type=jnp.float32)


def both_heads(block):
    lane = lax.broadcasted_iota(jnp.int32, block.shape, 1)
    zero = jnp.zeros_like(block)
    return jnp.concatenate([jnp.where(lane < HEAD_DIM, block, zero), jnp.where(lane >= HEAD_DIM, block, zero)], axis=0)


def own_blocks(wide):
    return jnp.concatenate([wide[:HEAD_DIM, :QT], wide[HEAD_DIM:, QT:]], axis=0)


def attend_kernel(first_ref, last_ref, q_ref, k_ref, v_ref, mark_ref, penalty_ref, head_ref, wide_ref, log_ref, score_ref, acc_ref, aug_ref):
    pairs = q_ref.shape[1] // LANES
    blocks = q_ref.shape[0] // QT
    for pair in range(pairs):
        aug_ref[pair, :, :LANES] = k_ref[:, pair * LANES:(pair + 1) * LANES]
        aug_ref[pair, :, LANES:] = mark_ref[...]

    def query_block(i, carry):
        rows = pl.ds(pl.multiple_of(i * QT, QT), QT)
        low, high = first_ref[i], last_ref[i]
        penalty = penalty_ref[rows, :]
        penalty = jnp.concatenate([penalty, penalty], axis=0)
        queries = [
            jnp.concatenate([both_heads(q_ref[rows, p * LANES:(p + 1) * LANES]), penalty], axis=1)
            for p in range(pairs)
        ]

        def first_pass(j, best):
            keys = pl.ds(pl.multiple_of(j * KT, KT), KT)
            out = []
            for p in range(pairs):
                scores = nt(aug_ref[p, keys, :], queries[p])
                score_ref[p, pl.ds(pl.multiple_of((j - low) * KT, KT), KT), :] = scores
                out.append(jnp.maximum(best[p], jnp.max(scores.reshape(KT // 8, 8, 2 * QT), axis=0)))
            return tuple(out)

        start = tuple(jnp.full((8, 2 * QT), -3e38, jnp.float32) for _ in range(pairs))
        best = lax.fori_loop(low, high, first_pass, start)
        best = [jnp.max(b, axis=0, keepdims=True) for b in best]
        acc_ref[...] = jnp.zeros_like(acc_ref)

        def second_pass(j, total):
            keys = pl.ds(pl.multiple_of(j * KT, KT), KT)
            out = []
            for p in range(pairs):
                scores = score_ref[p, pl.ds(pl.multiple_of((j - low) * KT, KT), KT), :]
                weight = jnp.exp(scores - best[p])
                out.append(total[p] + jnp.sum(weight.reshape(KT // 8, 8, 2 * QT), axis=0))
                acc_ref[p] += tn(v_ref[keys, p * LANES:(p + 1) * LANES], weight.astype(jnp.bfloat16))
            return tuple(out)

        zero = tuple(jnp.zeros((8, 2 * QT), jnp.float32) for _ in range(pairs))
        total = lax.fori_loop(low, high, second_pass, zero)
        for p in range(pairs):
            denom = jnp.sum(total[p], axis=0, keepdims=True)
            log_total = best[p] + jnp.log(denom)
            log_ref[2 * p:2 * p + 1, rows] = log_total[:, :QT]
            log_ref[2 * p + 1:2 * p + 2, rows] = log_total[:, QT:]
            mixed = own_blocks(acc_ref[p] / denom).T
            wide_ref[rows, p * LANES:(p + 1) * LANES] = mixed
            head_ref[rows, p * LANES:(p + 1) * LANES] = mixed.astype(jnp.bfloat16)
        return carry

    lax.fori_loop(0, blocks, query_block, 0)


def vmem():
    return pl.BlockSpec(memory_space=pltpu.VMEM)


def smem():
    return pl.BlockSpec(memory_space=pltpu.SMEM)


def cost(flops, moved):
    return pl.CostEstimate(flops=flops, bytes_accessed=moved, transcendentals=0)


def attend(first, last, q, k, v, mark, penalty):
    tokens, width = q.shape
    pairs = width // LANES
    return pl.pallas_call(
        attend_kernel,
        out_shape=(
            jax.ShapeDtypeStruct((tokens, width), jnp.bfloat16),
            jax.ShapeDtypeStruct((tokens, width), jnp.float32),
            jax.ShapeDtypeStruct((2 * pairs, tokens), jnp.float32),
        ),
        in_specs=[smem(), smem()] + [vmem()] * 5,
        out_specs=(vmem(), vmem(), vmem()),
        scratch_shapes=[
            pltpu.VMEM((pairs, tokens, 2 * QT), jnp.float32),
            pltpu.VMEM((pairs, LANES, 2 * QT), jnp.float32),
            pltpu.VMEM((pairs, tokens, 2 * LANES), jnp.bfloat16),
        ],
        name="attend",
        cost_estimate=pl.CostEstimate(flops=2 * 10**9, bytes_accessed=8 * 2**20, transcendentals=0),
    )(first, last, q, k, v, mark, penalty)


def turn(values):
    lane = lax.broadcasted_iota(jnp.int32, values.shape, 1)
    quarter = HEAD_DIM // 2
    ahead = pltpu.roll(values, LANES - quarter, 1)
    behind = pltpu.roll(values, quarter, 1)
    return jnp.where(lane % HEAD_DIM < quarter, ahead, behind)


def attend_back_kernel(first_ref, last_ref, q_ref, k_ref, v_ref, mark_ref, penalty_ref, wide_ref, log_ref, cot_ref, cos_ref, sin_ref,
                       dq_ref, dk_ref, dv_ref, aug_ref, dkey_ref, dval_ref, dqry_ref):
    pairs = q_ref.shape[1] // LANES
    blocks = q_ref.shape[0] // QT
    for pair in range(pairs):
        aug_ref[pair, :, :LANES] = k_ref[:, pair * LANES:(pair + 1) * LANES]
        aug_ref[pair, :, LANES:] = mark_ref[...]
    dkey_ref[...] = jnp.zeros_like(dkey_ref)
    dval_ref[...] = jnp.zeros_like(dval_ref)

    def query_block(i, carry):
        rows = pl.ds(pl.multiple_of(i * QT, QT), QT)
        low, high = first_ref[i], last_ref[i]
        penalty = penalty_ref[rows, :]
        penalty = jnp.concatenate([penalty, penalty], axis=0)
        plain, queries, cots, logs, deltas = [], [], [], [], []
        for p in range(pairs):
            lanes = slice(p * LANES, (p + 1) * LANES)
            block = both_heads(q_ref[rows, lanes])
            plain.append(block)
            queries.append(jnp.concatenate([block, penalty], axis=1))
            cot = cot_ref[rows, lanes]
            cots.append(both_heads(cot))
            product = (cot.astype(jnp.float32) * wide_ref[rows, lanes]).T
            deltas.append(jnp.concatenate(
                [jnp.sum(product[:HEAD_DIM], axis=0, keepdims=True), jnp.sum(product[HEAD_DIM:], axis=0, keepdims=True)], axis=1))
            logs.append(jnp.concatenate([log_ref[2 * p:2 * p + 1, rows], log_ref[2 * p + 1:2 * p + 2, rows]], axis=1))
        dqry_ref[...] = jnp.zeros_like(dqry_ref)

        def key_block(j, inner):
            keys = pl.ds(pl.multiple_of(j * KT, KT), KT)
            for p in range(pairs):
                lanes = slice(p * LANES, (p + 1) * LANES)
                prob = jnp.exp(nt(aug_ref[p, keys, :], queries[p]) - logs[p])
                grad_prob = nt(v_ref[keys, lanes], cots[p])
                grad_raw = (prob * (grad_prob - deltas[p])).astype(jnp.bfloat16)
                dval_ref[keys, lanes] += nn(prob.astype(jnp.bfloat16), cots[p])
                dkey_ref[keys, lanes] += nn(grad_raw, plain[p])
                dqry_ref[p] += tn(k_ref[keys, lanes], grad_raw)
            return inner

        lax.fori_loop(low, high, key_block, 0)
        cosine, sine = cos_ref[rows, :], sin_ref[rows, :]
        for p in range(pairs):
            grad = own_blocks(dqry_ref[p]).T * (HEAD_DIM ** -0.5)
            dq_ref[rows, p * LANES:(p + 1) * LANES] = (grad * cosine - turn(grad) * sine).astype(jnp.bfloat16)
        return carry

    lax.fori_loop(0, blocks, query_block, 0)

    def finish(i, carry):
        rows = pl.ds(pl.multiple_of(i * QT, QT), QT)
        cosine, sine = cos_ref[rows, :], sin_ref[rows, :]
        for p in range(pairs):
            lanes = slice(p * LANES, (p + 1) * LANES)
            grad = dkey_ref[rows, lanes]
            dk_ref[rows, lanes] = (grad * cosine - turn(grad) * sine).astype(jnp.bfloat16)
            dv_ref[rows, lanes] = dval_ref[rows, lanes].astype(jnp.bfloat16)
        return carry

    lax.fori_loop(0, blocks, finish, 0)


def attend_back(first, last, q, k, v, mark, penalty, wide, logs, cot, cosine, sine):
    tokens, width = q.shape
    pairs = width // LANES
    out = jax.ShapeDtypeStruct((tokens, width), jnp.bfloat16)
    return pl.pallas_call(
        attend_back_kernel,
        out_shape=(out, out, out),
        in_specs=[smem(), smem()] + [vmem()] * 10,
        out_specs=(vmem(),) * 3,
        scratch_shapes=[
            pltpu.VMEM((pairs, tokens, 2 * LANES), jnp.bfloat16),
            pltpu.VMEM((tokens, width), jnp.float32),
            pltpu.VMEM((tokens, width), jnp.float32),
            pltpu.VMEM((pairs, LANES, 2 * QT), jnp.float32),
        ],
        name="attend_back",
        cost_estimate=pl.CostEstimate(flops=5 * 10**9, bytes_accessed=16 * 2**20, transcendentals=0),
    )(first, last, q, k, v, mark, penalty, wide, logs, cot, cosine, sine)


def swap(values, bit, axis="mp"):
    size = lax.axis_size(axis)
    return lax.ppermute(values, axis, [(i, i ^ bit) for i in range(size)])


def gather_pieces(own):
    across = swap(own, 2)
    beside = swap(own, 1)
    return [own, beside, across, swap(across, 1)]


def scatter_sum(term, after=None):
    far = swap(term(3), 1)
    pair = (term(2).astype(jnp.float32) + far.astype(jnp.float32)).astype(jnp.bfloat16)
    if after is not None:
        pair, _ = lax.optimization_barrier((pair, after))
    cross = swap(pair, 2)
    near = swap(term(1), 1)
    return term(0).astype(jnp.float32) + near.astype(jnp.float32) + cross.astype(jnp.float32)


def reduce_dp(values, order):
    place = lax.axis_index("dp")
    bits = []
    while 1 << len(bits) < lax.axis_size("dp"):
        bits.append(1 << len(bits))
    bits = bits[order:] + bits[:order]
    for bit in bits:
        half = values.shape[0] // 2
        high = lax.bitwise_and(place, bit) // bit
        keep = lax.dynamic_slice_in_dim(values, high * half, half, 0)
        send = lax.dynamic_slice_in_dim(values, (1 - high) * half, half, 0)
        got = swap(send, bit, "dp")
        values = (keep.astype(jnp.float32) + got.astype(jnp.float32)).astype(jnp.bfloat16)
    for bit in reversed(bits):
        high = lax.bitwise_and(place, bit)
        other = swap(values, bit, "dp")
        values = jnp.where(high == 0, jnp.concatenate([values, other]), jnp.concatenate([other, values]))
    return values


def sum_all(values):
    for axis in ("mp", "dp"):
        bit = 1
        while bit < lax.axis_size(axis):
            values = values + swap(values, bit, axis)
            bit *= 2
    return values


def place_of(index_ref, j, rows):
    return pl.ds(pl.multiple_of(lax.bitwise_xor(index_ref[0], j) * rows, rows), rows)


def project_kernel(index_ref, a_ref, b_ref, c_ref, d_ref, weight_ref, cos_ref, sin_ref, q_ref, k_ref, v_ref):
    rows = a_ref.shape[0]
    width = q_ref.shape[1]
    for j, piece in enumerate((a_ref, b_ref, c_ref, d_ref)):
        place = place_of(index_ref, j, rows)
        cosine, sine = cos_ref[place, :], sin_ref[place, :]
        product = nn(piece[...], weight_ref[...])
        for out, base, scale in ((q_ref, 0, HEAD_DIM**-0.5), (k_ref, width, None)):
            for p in range(width // LANES):
                part = product[:, base + p * LANES : base + (p + 1) * LANES]
                turned = part * cosine + turn(part) * sine
                if scale is not None:
                    turned = turned * scale
                out[place, p * LANES : (p + 1) * LANES] = turned.astype(jnp.bfloat16)
        v_ref[place, :] = product[:, 2 * width :].astype(jnp.bfloat16)


def project(index, pieces, weight, cosine, sine):
    tokens = cosine.shape[0]
    width = weight.shape[1] // 3
    out = jax.ShapeDtypeStruct((tokens, width), jnp.bfloat16)
    return pl.pallas_call(
        project_kernel,
        out_shape=(out, out, out),
        in_specs=[smem()] + [vmem()] * 7,
        out_specs=(vmem(),) * 3,
        name="project",
        cost_estimate=cost(2 * tokens * weight.shape[0] * weight.shape[1], 10 * 2**20),
    )(index, *pieces, weight, cosine, sine)


def head_back_kernel(index_ref, a_ref, b_ref, c_ref, d_ref, weight_ref, out_ref):
    rows = a_ref.shape[0]
    for j, piece in enumerate((a_ref, b_ref, c_ref, d_ref)):
        out_ref[place_of(index_ref, j, rows), :] = nt(piece[...], weight_ref[...]).astype(jnp.bfloat16)


def head_back(index, pieces, weight):
    tokens = 4 * pieces[0].shape[0]
    return pl.pallas_call(
        head_back_kernel,
        out_shape=jax.ShapeDtypeStruct((tokens, weight.shape[0]), jnp.bfloat16),
        in_specs=[smem()] + [vmem()] * 5,
        out_specs=vmem(),
        name="head_back",
        cost_estimate=cost(2 * tokens * weight.shape[0] * weight.shape[1], 6 * 2**20),
    )(index, *pieces, weight)


def weight_grad_kernel(many, index_ref, *refs):
    lefts, rights = refs[: many[0]], [refs[many[0] + many[1] * r : many[0] + many[1] * (r + 1)] for r in range(many[2])]
    outs = refs[many[0] + many[1] * many[2] :]
    rows = lefts[0].shape[0] if many[0] == 4 else lefts[0].shape[0] // 4
    totals = [None] * len(rights)
    for j in range(4):
        place = place_of(index_ref, j, rows)
        left = lefts[j][...] if many[0] == 4 else lefts[0][place, :]
        for n, right in enumerate(rights):
            part = tn(left, right[j][...] if many[1] == 4 else right[0][place, :])
            totals[n] = part if totals[n] is None else totals[n] + part
    if len(outs) == 1:
        outs[0][...] = jnp.concatenate(totals, axis=1).astype(jnp.bfloat16)
    else:
        for out, total in zip(outs, totals):
            out[...] = total.astype(jnp.bfloat16)


def weight_grad(index, lefts, rights, tile, join=False):
    many = (len(lefts), len(rights[0]), len(rights))
    left_rows, depth = lefts[0].shape
    flat = [array for right in rights for array in right]
    wide = sum(right[0].shape[1] for right in rights)
    outs = tuple(jax.ShapeDtypeStruct((depth, right[0].shape[1]), jnp.bfloat16) for right in rights)
    if join:
        outs = (jax.ShapeDtypeStruct((depth, wide), jnp.bfloat16),)
    tokens = left_rows * (4 // len(lefts))
    return pl.pallas_call(
        functools.partial(weight_grad_kernel, many),
        grid=(depth // tile,),
        out_shape=outs,
        in_specs=[smem()]
        + [pl.BlockSpec((left_rows, tile), lambda i: (0, i))] * len(lefts)
        + [pl.BlockSpec(array.shape, lambda i: (0, 0)) for array in flat],
        out_specs=tuple(pl.BlockSpec((tile, o.shape[1]), lambda i: (i, 0)) for o in outs),
        cost_estimate=cost(2 * tokens * depth * wide, 2 * (tokens * (depth + wide) + depth * wide)),
    )(index, *lefts, *flat)


def spread_kernel(count, flip, targets, index_ref, *refs):
    arrays, weights, outs = refs[:count], refs[count : 2 * count], refs[2 * count :]
    rows = arrays[0].shape[0] // 4
    product = nt if flip else nn
    for out, j in zip(outs, targets):
        place = place_of(index_ref, j, rows)
        total = product(arrays[0][place, :], weights[0][...])
        for array, weight in zip(arrays[1:], weights[1:]):
            total = total + product(array[place, :], weight[...])
        out[...] = total.astype(jnp.bfloat16)


def spread(index, arrays, weights, flip, targets):
    tokens, depth = arrays[0].shape
    width = weights[0].shape[0 if flip else 1]
    count = len(arrays)
    out = jax.ShapeDtypeStruct((tokens // 4, width), jnp.bfloat16)
    return pl.pallas_call(
        functools.partial(spread_kernel, count, flip, targets),
        out_shape=(out,) * len(targets),
        in_specs=[smem()] + [vmem()] * (2 * count),
        out_specs=(vmem(),) * len(targets),
        cost_estimate=cost(2 * count * len(targets) * (tokens // 4) * depth * width, 2 * 2**20 * len(targets)),
    )(index, *arrays, *weights)


def feed_kernel(count, *refs):
    inputs, cots = refs[:count], refs[count : 2 * count]
    gate_w, up_w, down_w = refs[2 * count : 2 * count + 3]
    outs = refs[2 * count + 3 :]
    for j in range(count):
        normed = inputs[j][...]
        gate = nn(normed, gate_w[...])
        up = nn(normed, up_w[...])
        grad = nt(cots[j][...], down_w[...])
        sig = jax.nn.sigmoid(gate)
        silu = gate * sig
        outs[j][...] = (silu * up).astype(jnp.bfloat16)
        outs[count + j][...] = (grad * up * (sig + silu * (1.0 - sig))).astype(jnp.bfloat16)
        outs[2 * count + j][...] = (grad * silu).astype(jnp.bfloat16)


def feed(inputs, cots, gate_w, up_w, down_w, tile=256):
    count = len(inputs)
    rows, width = inputs[0].shape
    hidden = gate_w.shape[1]
    out = jax.ShapeDtypeStruct((rows, hidden), jnp.bfloat16)
    whole = pl.BlockSpec((rows, width), lambda i: (0, 0))
    column = pl.BlockSpec((width, tile), lambda i: (0, i))
    outs = pl.pallas_call(
        functools.partial(feed_kernel, count),
        grid=(hidden // tile,),
        out_shape=(out,) * (3 * count),
        in_specs=[whole] * (2 * count) + [column, column, pl.BlockSpec((tile, width), lambda i: (i, 0))],
        out_specs=(pl.BlockSpec((rows, tile), lambda i: (0, i)),) * (3 * count),
        name="feed",
        cost_estimate=cost(6 * count * rows * width * hidden, 2 * (3 * width * hidden + count * rows * (2 * width + 3 * hidden))),
    )(*inputs, *cots, gate_w, up_w, down_w)
    return outs[:count], outs[count : 2 * count], outs[2 * count :]


def normalize(values):
    center = values - jnp.mean(values, axis=-1, keepdims=True)
    inverse = lax.rsqrt(jnp.mean(center * center, axis=-1, keepdims=True) + epsilon)
    return (center * inverse, inverse)


def norm_back(incoming, scaled, inverse, gain):
    gain_part = jnp.sum(incoming * scaled, axis=0)
    shift_part = jnp.sum(incoming, axis=0)
    along = incoming * gain
    mean_plain = jnp.mean(along, axis=-1, keepdims=True)
    mean_mixed = jnp.mean(along * scaled, axis=-1, keepdims=True)
    return (inverse * (along - mean_plain - scaled * mean_mixed), gain_part, shift_part)


def window_plan(seg):
    tokens = seg.shape[0]
    heads = seg[::QT]
    tails = seg[QT - 1 :: QT]
    begin = jnp.sum((seg[None, :] < heads[:, None]).astype(jnp.int32), axis=1)
    end = jnp.sum((seg[None, :] <= tails[:, None]).astype(jnp.int32), axis=1)
    first = begin // KT
    last = (end + KT - 1) // KT
    number = lax.broadcasted_iota(jnp.int32, (tokens, LANES), 1)
    same = seg[:, None] == number
    mark = same.astype(jnp.bfloat16)
    penalty = jnp.where(same, 0.0, -1e30).astype(jnp.bfloat16)
    opening = jnp.sum((seg[:, None] < number).astype(jnp.int32), axis=0)
    start = jnp.sum(jnp.where(same, opening[None, :], 0), axis=1)
    position = (jnp.arange(tokens, dtype=jnp.int32) - start).astype(jnp.float32)
    half_dim = HEAD_DIM // 2
    frequency = 10000.0 ** (-2.0 * jnp.arange(half_dim, dtype=jnp.float32) / HEAD_DIM)
    angles = position[:, None] * jnp.tile(frequency, LANES // half_dim)[None, :]
    sign = jnp.where(jnp.arange(LANES) % HEAD_DIM < half_dim, -1.0, 1.0)
    cosine, sine = jnp.cos(angles), jnp.sin(angles) * sign[None, :]
    return first, last, mark, penalty, cosine, sine


def layer(
    tokens,
    segments,
    attn_norm_gain,
    attn_norm_bias,
    query_weight,
    key_weight,
    value_weight,
    output_weight,
    mlp_norm_gain,
    mlp_norm_bias,
    gate_weight,
    up_weight,
    down_weight,
    grad_out,
):
    position = lax.axis_index("mp")
    index = position.astype(jnp.int32).reshape(1)
    first, last, mark, penalty, cosine, sine = window_plan(segments.reshape(-1))

    inputs = tokens.astype(jnp.float32)
    attn_scaled, attn_inverse = normalize(inputs)
    attn_normed = (attn_scaled * attn_norm_gain + attn_norm_bias).astype(jnp.bfloat16)
    attn_pieces = gather_pieces(attn_normed)
    qkv_weight = jnp.concatenate([query_weight, key_weight, value_weight], axis=1)
    query_rot, key_rot, value_low = project(index, attn_pieces, qkv_weight, cosine, sine)
    late_cot, _ = lax.optimization_barrier((grad_out, attn_pieces[2]))
    cot_pieces = gather_pieces(late_cot)
    head_out, head_wide, log_totals = attend(first, last, query_rot, key_rot, value_low, mark, penalty)
    outward = spread(index, [head_out], [output_weight], False, (3, 2))
    inward = spread(index, [head_out], [output_weight], False, (1, 0))
    middle = inputs + scatter_sum([inward[1], inward[0], outward[1], outward[0]].__getitem__)
    mlp_scaled, mlp_inverse = normalize(middle)
    mlp_normed = (mlp_scaled * mlp_norm_gain + mlp_norm_bias).astype(jnp.bfloat16)
    mlp_pieces = gather_pieces(mlp_normed)
    near = feed(mlp_pieces[:2], cot_pieces[:2], gate_weight, up_weight, down_weight)
    far = feed(mlp_pieces[2:], cot_pieces[2:], gate_weight, up_weight, down_weight)
    hidden, grad_gate, grad_up = [list(a) + list(b) for a, b in zip(near, far)]
    grad_mlp_normed = scatter_sum(
        lambda j: (nt(grad_gate[j], gate_weight) + nt(grad_up[j], up_weight)).astype(jnp.bfloat16)
    )
    (grad_down,) = weight_grad(index, hidden, [cot_pieces], 256)
    grad_gate_w, grad_up_w = weight_grad(index, mlp_pieces, [grad_gate, grad_up], 256)
    summed_gate, summed_up, summed_down = lax.psum((grad_gate_w, grad_up_w, grad_down), "dp")
    middle_part, mlp_gain_part, mlp_shift_part = norm_back(grad_mlp_normed, mlp_scaled, mlp_inverse, mlp_norm_gain)
    grad_middle = grad_out.astype(jnp.float32) + middle_part
    attn_cot = gather_pieces(grad_middle.astype(jnp.bfloat16))
    grad_head = head_back(index, attn_cot, output_weight)
    block_out = (
        middle
        + scatter_sum(
            lambda j: jnp.dot(hidden[j], down_weight, preferred_element_type=jnp.float32).astype(jnp.bfloat16),
            attn_cot[2],
        )
    ).astype(jnp.bfloat16)
    (grad_output_w,) = weight_grad(index, attn_cot, [[head_out]], 256, True)
    grad_query, grad_key, grad_value = attend_back(
        first, last, query_rot, key_rot, value_low, mark, penalty, head_wide, log_totals, grad_head, cosine, sine
    )
    first_part, second_part = weight_grad(
        index, attn_pieces, [[grad_query], [grad_key], [grad_value]], 256, True
    )[0], grad_output_w
    width = grad_query.shape[1]
    second_part = jnp.concatenate([first_part[:, 2 * width :], second_part], axis=1)
    first_part = reduce_dp(first_part[:, : 2 * width], 0)
    second_part = reduce_dp(second_part, 1)
    qkv = [grad_query, grad_key, grad_value], [query_weight, key_weight, value_weight]
    outward = spread(index, *qkv, True, (3, 2))
    inward = spread(index, *qkv, True, (1, 0))
    grad_attn_normed = scatter_sum([inward[1], inward[0], outward[1], outward[0]].__getitem__)
    input_part, attn_gain_part, attn_shift_part = norm_back(grad_attn_normed, attn_scaled, attn_inverse, attn_norm_gain)
    grad_tokens = grad_middle + input_part
    sums = sum_all(jnp.stack([attn_gain_part, attn_shift_part, mlp_gain_part, mlp_shift_part]))

    def wide(values):
        return values.astype(jnp.float32)

    return (
        block_out,
        grad_tokens,
        sums[0],
        sums[1],
        wide(first_part[:, :width]),
        wide(first_part[:, width:]),
        wide(second_part[:, :width]),
        wide(second_part[:, width:].T),
        sums[2],
        sums[3],
        wide(summed_gate),
        wide(summed_up),
        wide(summed_down),
    )


def solution(mesh):
    in_specs = (
        P(("dp", "mp"), None),
        P("dp", None),
        P(),
        P(),
        P(None, "mp"),
        P(None, "mp"),
        P(None, "mp"),
        P("mp", None),
        P(),
        P(),
        P(None, "mp"),
        P(None, "mp"),
        P("mp", None),
        P(("dp", "mp"), None),
    )
    out_specs = (
        P(("dp", "mp"), None),
        P(("dp", "mp"), None),
        P(),
        P(),
        P(None, "mp"),
        P(None, "mp"),
        P(None, "mp"),
        P("mp", None),
        P(),
        P(),
        P(None, "mp"),
        P(None, "mp"),
        P("mp", None),
    )
    return jax.shard_map(layer, mesh=mesh, in_specs=in_specs, out_specs=out_specs, check_vma=False)
```
